32 devices in a mesh: block: 4 (over x, core), span: 4 (over z), model: 2 (over y).
Axes of the slice: x: 2, y: 2, z: 4, core: 2. Of those that a mesh axis runs over, the one named last changes fastest.
Arguments:
- fresh_keys: bfloat16 [16, 8192, 8, 128], P(None, ('block', 'span'), 'model'), may hold values from -6 to 6
- fresh_values: bfloat16 [16, 8192, 8, 128], P(None, ('block', 'span'), 'model'), may hold values from -6 to 6
- turn_angle: float32 [8192, 64], replicated, may hold values from -3.140625 to 3.140625
Outputs:
- decode_keys: bfloat16 [16, 8, 128, 8192], P(('block', 'span'), 'model')
- decode_values: bfloat16 [16, 8192, 8, 128], P(('block', 'span'), None, 'model')
- page_high: bfloat16 [16, 128, 8, 128], P(('block', 'span'), None, 'model')
- page_low: bfloat16 [16, 128, 8, 128], P(('block', 'span'), None, 'model')
The draws below stay inside these ranges and needn't reach their ends.
All inputs are finite; a program needn't handle non-finite values.
Results may differ from the reference program's by a relative error of at most 0.001.
Values may be sent and summed in bfloat16 or wider, within the bound.
A program may use at most 128 MiB of HBM per device.

```python
import jax
import jax.numpy as jnp

BATCH = 16
LENGTH = 8192
KV_HEADS = 8
HEAD_SIZE = 128
HALF_HEAD = 64
PAGE = 64


def level_of(own_key, dims, split, smallest, high):
    def one(axis_at, blocks):
        draws = jax.random.uniform(jax.random.fold_in(jax.random.fold_in(own_key, 6), axis_at), (blocks,), jnp.float32, smallest / len(split), high / len(split))
        return jnp.repeat(jnp.exp(draws), dims[axis_at] // blocks).reshape((-1,) + (1,) * (len(dims) - axis_at - 1))

    gain = one(*split[0])
    for cut in split[1:]:
        gain = gain * one(*cut)
    return gain


def noise(stream_key, shape, deviation, most, split=(), held_as=jnp.bfloat16):
    result = deviation * jax.random.normal(stream_key, shape, jnp.float32)
    if split:
        result = result * level_of(stream_key, shape, split, -0.22, 0.18)
    return jnp.clip(result, -most, most).astype(held_as)


def setup_inputs(seed: int = 0) -> dict:
    seeds = jax.random.split(jax.random.key(seed), 4)
    return {
        "fresh_keys": noise(seeds[0], (BATCH, LENGTH, KV_HEADS, HEAD_SIZE), 1.0, 6.0, ((1, 16), (2, 2))),
        "fresh_values": noise(seeds[1], (BATCH, LENGTH, KV_HEADS, HEAD_SIZE), 1.0, 6.0, ((1, 16), (2, 2))),
        "turn_angle": jnp.clip(jax.random.uniform(seeds[2], (LENGTH, HALF_HEAD), jnp.float32, -3.140625, 3.140625), -3.140625, 3.140625),
    }


def apply_rotary(vectors, angle):
    half = vectors.shape[-1] // 2
    cosine, sine = jnp.cos(angle)[None, :, None, :], jnp.sin(angle)[None, :, None, :]
    first, second = vectors[..., :half], vectors[..., half:]
    return jnp.concatenate([first * cosine - second * sine, second * cosine + first * sine], axis=-1)


def ready_to_store(plain_keys, angle):
    wide_keys = plain_keys.astype(jnp.float32)
    return apply_rotary(wide_keys, angle)


def reference(fresh_keys, fresh_values, turn_angle):
    turned_keys = ready_to_store(fresh_keys, turn_angle)
    narrow_keys = turned_keys.astype(jnp.bfloat16)
    page_view = narrow_keys.reshape(BATCH, LENGTH // PAGE, PAGE, KV_HEADS, HEAD_SIZE)
    page_high = jnp.max(page_view, axis=2)
    page_low = jnp.min(page_view, axis=2)
    decode_keys = jnp.transpose(narrow_keys, (0, 2, 3, 1))
    decode_values = fresh_values
    return decode_keys, decode_values, page_high, page_low
```

```python
import functools

import jax
import jax.numpy as jnp
from jax import lax
from jax.experimental import pallas as pl
from jax.experimental.pallas import tpu as pltpu
from jax.sharding import PartitionSpec as P

PAGE = 64
ROWS = 256


def kernel(
    dims, keys, values, angle,
    out_keys, out_values, out_high, out_low,
    held, landed, wide, cosine, sine, turn, staged, bounds, own,
    send_v, recv_v, send_k, recv_k, load_sem, own_sem, stage_sem,
):
    spans, n, seqs, length, heads, size = dims
    rows = length * heads
    pages = length // PAGE
    block, span, model = (lax.axis_index(a) for a in ("block", "span", "model"))
    me = block * spans + span

    def peer(j):
        return (j // spans, lax.rem(j, spans), model)

    def send_values(j):
        return pltpu.make_async_remote_copy(
            src_ref=values.at[pl.ds(j * seqs, seqs)],
            dst_ref=out_values.at[:, me],
            send_sem=send_v.at[j],
            recv_sem=recv_v.at[me],
            device_id=peer(j),
            device_id_type=pl.DeviceIdType.MESH,
        )

    def recv_values(j):
        return pltpu.make_async_remote_copy(
            src_ref=values.at[pl.ds(j * seqs, seqs)],
            dst_ref=out_values.at[:, j],
            send_sem=send_v.at[j],
            recv_sem=recv_v.at[j],
            device_id=peer(j),
            device_id_type=pl.DeviceIdType.MESH,
        )

    def send_keys(j):
        return pltpu.make_async_remote_copy(
            src_ref=held.at[pl.ds(j * seqs, seqs)],
            dst_ref=landed.at[pl.ds(me * seqs, seqs)],
            send_sem=send_k.at[j],
            recv_sem=recv_k.at[me],
            device_id=peer(j),
            device_id_type=pl.DeviceIdType.MESH,
        )

    def recv_keys(j):
        return pltpu.make_async_remote_copy(
            src_ref=held.at[pl.ds(j * seqs, seqs)],
            dst_ref=landed.at[pl.ds(j * seqs, seqs)],
            send_sem=send_k.at[j],
            recv_sem=recv_k.at[j],
            device_id=peer(j),
            device_id_type=pl.DeviceIdType.MESH,
        )

    load_keys = pltpu.make_async_copy(keys, held, load_sem.at[0])
    load_angle = pltpu.make_async_copy(
        angle.at[:, pl.ds(pl.multiple_of(me * length, length), length)], turn, load_sem.at[1]
    )
    load_own = pltpu.make_async_copy(values.at[pl.ds(me * seqs, seqs)], own, own_sem.at[0])
    keep_own = pltpu.make_async_copy(own, out_values.at[:, me], own_sem.at[1])
    load_angle.start()
    load_keys.start()
    load_own.start()

    barrier = pltpu.get_barrier_semaphore()

    @pl.loop(1, n)
    def _(k):
        pl.semaphore_signal(
            barrier, inc=1, device_id=peer(lax.rem(me + k, n)),
            device_id_type=pl.DeviceIdType.MESH,
        )

    pl.semaphore_wait(barrier, n - 1)

    @pl.loop(1, n)
    def _(k):
        send_values(lax.rem(me + k, n)).start()

    load_angle.wait()
    c, s = jnp.cos(turn[...]), jnp.sin(turn[...])
    wide_c = jnp.concatenate([c, c], axis=0).T
    wide_s = jnp.concatenate([-s, s], axis=0).T
    for h in range(heads):
        cosine[pl.ds(h, length, stride=heads), :] = wide_c
        sine[pl.ds(h, length, stride=heads), :] = wide_s
    load_own.wait()
    keep_own.start()
    load_keys.wait()

    def rotate(j):
        for q in range(seqs):

            @pl.loop(0, rows // ROWS)
            def _(r):
                at = pl.ds(pl.multiple_of(r * ROWS, ROWS), ROWS)
                x = held[j * seqs + q, at, :].astype(jnp.float32)
                y = x * cosine[at, :] + pltpu.roll(x, size // 2, 1) * sine[at, :]
                held[j * seqs + q, at, :] = y.astype(jnp.bfloat16)

    rotate(lax.rem(me + 1, n))

    @pl.loop(2, n + 1)
    def _(k):
        rotate(lax.rem(me + k, n))
        send_keys(lax.rem(me + k - 1, n)).start()

    keep_own.wait()

    def stage(j, q, slot):
        return pltpu.make_async_copy(
            staged.at[slot],
            out_keys.at[q, :, :, pl.ds(pl.multiple_of(j * length, length), length)],
            stage_sem.at[slot],
        )

    def finish(ref, row, j, q, slot, first):
        wide[...] = ref[row].astype(jnp.float32)

        @pl.when(jnp.logical_not(first))
        def _():
            stage(j, q, slot).wait()

        for h in range(heads):
            part = wide[pl.ds(h, length, stride=heads), :]
            staged[slot, h] = part.T.astype(jnp.bfloat16)
            grouped = part.reshape(pages, PAGE, size)
            bounds[0, pl.ds(h, pages, stride=heads), :] = jnp.max(grouped, axis=1)
            bounds[1, pl.ds(h, pages, stride=heads), :] = jnp.min(grouped, axis=1)
        out_high[q, j] = bounds[0].astype(jnp.bfloat16)
        out_low[q, j] = bounds[1].astype(jnp.bfloat16)
        stage(j, q, slot).start()

    total = n * seqs
    for q in range(seqs):
        finish(held, me * seqs + q, me, q, q % 2, jnp.bool_(q < 2))

    @pl.loop(1, n)
    def _(k):
        j = lax.rem(me + n - k, n)
        recv_keys(j).wait_recv()
        for q in range(seqs):
            step = k * seqs + q
            finish(landed, j * seqs + q, j, q, lax.rem(step, 2), step < 2)

    for last in range(max(0, total - 2), total):
        stage(0, 0, last % 2).wait()

    @pl.loop(1, n)
    def _(k):
        j = lax.rem(me + k, n)
        send_values(j).wait_send()
        send_keys(j).wait_send()

    @pl.loop(1, n)
    def _(k):
        recv_values(lax.rem(me + n - k, n)).wait_recv()


def body(mesh, fresh_keys, fresh_values, turn_angle):
    spans = mesh.shape["span"]
    n = mesh.shape["block"] * spans
    batch, length, heads, size = fresh_keys.shape
    seqs = batch // n
    rows = length * heads
    pages = length // PAGE
    flat = (batch, rows, size)
    hbm = pl.BlockSpec(memory_space=pltpu.HBM)
    vmem = pl.BlockSpec(memory_space=pltpu.VMEM)
    keys, values, high, low = pl.pallas_call(
        functools.partial(kernel, (spans, n, seqs, length, heads, size)),
        out_shape=(
            jax.ShapeDtypeStruct((seqs, heads, size, n * length), jnp.bfloat16),
            jax.ShapeDtypeStruct((seqs, n, rows, size), jnp.bfloat16),
            jax.ShapeDtypeStruct((seqs, n, pages * heads, size), jnp.bfloat16),
            jax.ShapeDtypeStruct((seqs, n, pages * heads, size), jnp.bfloat16),
        ),
        in_specs=[hbm] * 3,
        out_specs=(hbm, hbm, vmem, vmem),
        scratch_shapes=[
            pltpu.VMEM(flat, jnp.bfloat16),
            pltpu.VMEM(flat, jnp.bfloat16),
            pltpu.VMEM((rows, size), jnp.float32),
            pltpu.VMEM((rows, size), jnp.float32),
            pltpu.VMEM((rows, size), jnp.float32),
            pltpu.VMEM((size // 2, length), jnp.float32),
            pltpu.VMEM((2, heads, size, length), jnp.bfloat16),
            pltpu.VMEM((2, pages * heads, size), jnp.float32),
            pltpu.VMEM((seqs, rows, size), jnp.bfloat16),
            pltpu.SemaphoreType.DMA((n,)),
            pltpu.SemaphoreType.DMA((n,)),
            pltpu.SemaphoreType.DMA((n,)),
            pltpu.SemaphoreType.DMA((n,)),
            pltpu.SemaphoreType.DMA((2,)),
            pltpu.SemaphoreType.DMA((2,)),
            pltpu.SemaphoreType.DMA((2,)),
        ],
        compiler_params=pltpu.CompilerParams(
            collective_id=0, has_side_effects=True, vmem_limit_bytes=60 * 1024 * 1024
        ),
        name="exchange",
    )(fresh_keys.reshape(flat), fresh_values.reshape(flat), turn_angle.T)
    return (
        keys,
        values.reshape(seqs, n * length, heads, size),
        high.reshape(seqs, n * pages, heads, size),
        low.reshape(seqs, n * pages, heads, size),
    )


def solution(mesh):
    placed = (
        P(None, ("block", "span"), "model", None),
        P(None, ("block", "span"), "model", None),
        P(),
    )
    return jax.shard_map(
        functools.partial(body, mesh),
        mesh=mesh,
        in_specs=placed,
        out_specs=(
            P(("block", "span"), "model", None, None),
            P(("block", "span"), None, "model", None),
            P(("block", "span"), None, "model", None),
            P(("block", "span"), None, "model", None),
        ),
        check_vma=False,
    )
```

```python
import functools

import jax
import jax.numpy as jnp
from jax import lax
from jax.experimental import pallas as pl
from jax.experimental.pallas import tpu as pltpu
from jax.sharding import PartitionSpec as P

PAGE = 64
ROWS = 256
TAIL = 8


def kernel(
    dims, keys, values, angle,
    out_keys, out_values, out_high, out_low, out_late,
    held, landed, wide, cosine, sine, turn, staged, bounds, own, late,
    send_v, recv_v, send_k, recv_k, load_sem, own_sem, stage_sem,
):
    spans, n, seqs, length, heads, size = dims
    rows = length * heads
    pages = length // PAGE
    most = rows - rows // TAIL
    block, span, model = (lax.axis_index(a) for a in ("block", "span", "model"))
    me = block * spans + span

    def peer(j):
        return (j // spans, lax.rem(j, spans), model)

    def send_values(j):
        return pltpu.make_async_remote_copy(
            src_ref=values.at[pl.ds(j * seqs, seqs), pl.ds(0, most)],
            dst_ref=out_values.at[:, me],
            send_sem=send_v.at[j],
            recv_sem=recv_v.at[me],
            device_id=peer(j),
            device_id_type=pl.DeviceIdType.MESH,
        )

    def recv_values(j):
        return pltpu.make_async_remote_copy(
            src_ref=values.at[pl.ds(j * seqs, seqs), pl.ds(0, most)],
            dst_ref=out_values.at[:, j],
            send_sem=send_v.at[j],
            recv_sem=recv_v.at[j],
            device_id=peer(j),
            device_id_type=pl.DeviceIdType.MESH,
        )

    def send_keys(j):
        return pltpu.make_async_remote_copy(
            src_ref=held.at[pl.ds(j * seqs, seqs)],
            dst_ref=landed.at[pl.ds(me * seqs, seqs)],
            send_sem=send_k.at[j],
            recv_sem=recv_k.at[me],
            device_id=peer(j),
            device_id_type=pl.DeviceIdType.MESH,
        )

    def recv_keys(j):
        return pltpu.make_async_remote_copy(
            src_ref=held.at[pl.ds(j * seqs, seqs)],
            dst_ref=landed.at[pl.ds(j * seqs, seqs)],
            send_sem=send_k.at[j],
            recv_sem=recv_k.at[j],
            device_id=peer(j),
            device_id_type=pl.DeviceIdType.MESH,
        )

    load_keys = pltpu.make_async_copy(keys, held, load_sem.at[0])
    load_angle = pltpu.make_async_copy(
        angle.at[:, pl.ds(pl.multiple_of(me * length, length), length)], turn, load_sem.at[1]
    )
    load_own = pltpu.make_async_copy(values.at[pl.ds(me * seqs, seqs), pl.ds(0, most)], own, own_sem.at[0]
    )
    keep_own = pltpu.make_async_copy(own, out_values.at[:, me], own_sem.at[1])
    load_late = pltpu.make_async_copy(
        values.at[:, pl.ds(most, rows - most)], late, own_sem.at[2]
    )
    keep_late = pltpu.make_async_copy(late, out_late, own_sem.at[3])
    load_angle.start()
    load_keys.start()
    load_own.start()
    load_late.start()

    barrier = pltpu.get_barrier_semaphore()

    @pl.loop(1, n)
    def _(k):
        pl.semaphore_signal(
            barrier, inc=1, device_id=peer(lax.rem(me + k, n)),
            device_id_type=pl.DeviceIdType.MESH,
        )

    pl.semaphore_wait(barrier, n - 1)

    @pl.loop(1, n)
    def _(k):
        send_values(lax.rem(me + k, n)).start()

    load_angle.wait()
    c, s = jnp.cos(turn[...]), jnp.sin(turn[...])
    wide_c = jnp.concatenate([c, c], axis=0).T
    wide_s = jnp.concatenate([-s, s], axis=0).T
    for h in range(heads):
        cosine[pl.ds(h, length, stride=heads), :] = wide_c
        sine[pl.ds(h, length, stride=heads), :] = wide_s
    load_own.wait()
    keep_own.start()
    load_late.wait()
    keep_late.start()
    load_keys.wait()

    def rotate(j):
        for q in range(seqs):

            @pl.loop(0, rows // ROWS)
            def _(r):
                at = pl.ds(pl.multiple_of(r * ROWS, ROWS), ROWS)
                x = held[j * seqs + q, at, :].astype(jnp.float32)
                y = x * cosine[at, :] + pltpu.roll(x, size // 2, 1) * sine[at, :]
                held[j * seqs + q, at, :] = y.astype(jnp.bfloat16)

    rotate(lax.rem(me + 1, n))

    @pl.loop(2, n + 1)
    def _(k):
        rotate(lax.rem(me + k, n))
        send_keys(lax.rem(me + k - 1, n)).start()

    keep_own.wait()
    keep_late.wait()

    def stage(j, q, slot):
        return pltpu.make_async_copy(
            staged.at[slot],
            out_keys.at[q, :, :, pl.ds(pl.multiple_of(j * length, length), length)],
            stage_sem.at[slot],
        )

    def finish(ref, row, j, q, slot, first):
        wide[...] = ref[row].astype(jnp.float32)

        @pl.when(jnp.logical_not(first))
        def _():
            stage(j, q, slot).wait()

        for h in range(heads):
            part = wide[pl.ds(h, length, stride=heads), :]
            staged[slot, h] = part.T.astype(jnp.bfloat16)
            grouped = part.reshape(pages, PAGE, size)
            bounds[0, pl.ds(h, pages, stride=heads), :] = jnp.max(grouped, axis=1)
            bounds[1, pl.ds(h, pages, stride=heads), :] = jnp.min(grouped, axis=1)
        out_high[q, j] = bounds[0].astype(jnp.bfloat16)
        out_low[q, j] = bounds[1].astype(jnp.bfloat16)
        stage(j, q, slot).start()

    total = n * seqs
    for q in range(seqs):
        finish(held, me * seqs + q, me, q, q % 2, jnp.bool_(q < 2))

    @pl.loop(1, n)
    def _(k):
        j = lax.rem(me + n - k, n)
        recv_keys(j).wait_recv()
        for q in range(seqs):
            step = k * seqs + q
            finish(landed, j * seqs + q, j, q, lax.rem(step, 2), step < 2)

    for last in range(max(0, total - 2), total):
        stage(0, 0, last % 2).wait()

    @pl.loop(1, n)
    def _(k):
        j = lax.rem(me + k, n)
        send_values(j).wait_send()
        send_keys(j).wait_send()

    @pl.loop(1, n)
    def _(k):
        recv_values(lax.rem(me + n - k, n)).wait_recv()


def copy_kernel(keys, values, out_keys, out_values):
    out_keys[...] = keys[...]
    out_values[...] = values[...]


def late_kernel(_, late, out):
    out[...] = late[...]


def body(mesh, fresh_keys, fresh_values, turn_angle):
    spans = mesh.shape["span"]
    n = mesh.shape["block"] * spans
    batch, length, heads, size = fresh_keys.shape
    seqs = batch // n
    rows = length * heads
    pages = length // PAGE
    flat = (batch, rows, size)
    hbm = pl.BlockSpec(memory_space=pltpu.HBM)
    vmem = pl.BlockSpec(memory_space=pltpu.VMEM)
    most = rows - rows // TAIL
    keys, values, high, low, late = pl.pallas_call(
        functools.partial(kernel, (spans, n, seqs, length, heads, size)),
        out_shape=(
            jax.ShapeDtypeStruct((seqs, heads, size, n * length), jnp.bfloat16),
            jax.ShapeDtypeStruct((seqs, n, most, size), jnp.bfloat16),
            jax.ShapeDtypeStruct((seqs, n, pages * heads, size), jnp.bfloat16),
            jax.ShapeDtypeStruct((seqs, n, pages * heads, size), jnp.bfloat16),
            jax.ShapeDtypeStruct((batch, rows - most, size), jnp.bfloat16),
        ),
        in_specs=[hbm] * 3,
        out_specs=(hbm, hbm, vmem, vmem, hbm),
        scratch_shapes=[
            pltpu.VMEM(flat, jnp.bfloat16),
            pltpu.VMEM(flat, jnp.bfloat16),
            pltpu.VMEM((rows, size), jnp.float32),
            pltpu.VMEM((rows, size), jnp.float32),
            pltpu.VMEM((rows, size), jnp.float32),
            pltpu.VMEM((size // 2, length), jnp.float32),
            pltpu.VMEM((2, heads, size, length), jnp.bfloat16),
            pltpu.VMEM((2, pages * heads, size), jnp.float32),
            pltpu.VMEM((seqs, most, size), jnp.bfloat16),
            pltpu.VMEM((batch, rows - most, size), jnp.bfloat16),
            pltpu.SemaphoreType.DMA((n,)),
            pltpu.SemaphoreType.DMA((n,)),
            pltpu.SemaphoreType.DMA((n,)),
            pltpu.SemaphoreType.DMA((n,)),
            pltpu.SemaphoreType.DMA((2,)),
            pltpu.SemaphoreType.DMA((4,)),
            pltpu.SemaphoreType.DMA((2,)),
        ],
        compiler_params=pltpu.CompilerParams(
            collective_id=0, has_side_effects=True, vmem_limit_bytes=60 * 1024 * 1024
        ),
        name="exchange",
    )(fresh_keys.reshape(flat), fresh_values.reshape(flat), turn_angle.T)
    late = lax.all_to_all(late, ("block", "span"), split_axis=0, concat_axis=0, tiled=True)
    late = jnp.swapaxes(late.reshape(n, seqs, rows - most, size), 0, 1)
    keys, values = pl.pallas_call(
        copy_kernel,
        grid=(seqs, n),
        out_shape=(
            jax.ShapeDtypeStruct(keys.shape, keys.dtype),
            jax.ShapeDtypeStruct((seqs, n, rows, size), jnp.bfloat16),
        ),
        in_specs=[
            pl.BlockSpec((1, heads, size, length), lambda q, j: (q, 0, 0, j)),
            pl.BlockSpec((1, 1, most, size), lambda q, j: (q, j, 0, 0)),
        ],
        out_specs=(
            pl.BlockSpec((1, heads, size, length), lambda q, j: (q, 0, 0, j)),
            pl.BlockSpec((1, 1, most, size), lambda q, j: (q, j, 0, 0)),
        ),
        cost_estimate=pl.CostEstimate(
            flops=0, bytes_accessed=8 * seqs * n * rows * size, transcendentals=0
        ),
        name="keep",
    )(keys, values)
    values = pl.pallas_call(
        late_kernel,
        grid=(seqs, n),
        out_shape=jax.ShapeDtypeStruct(values.shape, values.dtype),
        in_specs=[
            pl.BlockSpec(memory_space=pltpu.HBM),
            pl.BlockSpec((1, 1, rows - most, size), lambda q, j: (q, j, 0, 0)),
        ],
        out_specs=pl.BlockSpec((1, 1, rows - most, size), lambda q, j: (q, j, TAIL - 1, 0)),
        input_output_aliases={0: 0},
        name="join",
    )(values, late)
    return (
        keys,
        values.reshape(seqs, n * length, heads, size),
        high.reshape(seqs, n * pages, heads, size),
        low.reshape(seqs, n * pages, heads, size),
    )


def solution(mesh):
    placed = (
        P(None, ("block", "span"), "model", None),
        P(None, ("block", "span"), "model", None),
        P(),
    )
    return jax.shard_map(
        functools.partial(body, mesh),
        mesh=mesh,
        in_specs=placed,
        out_specs=(
            P(("block", "span"), "model", None, None),
            P(("block", "span"), None, "model", None),
            P(("block", "span"), None, "model", None),
            P(("block", "span"), None, "model", None),
        ),
        check_vma=False,
    )
```
